8 devices in a mesh: dp: 2 (over z, y), sp: 4 (over x, core).
Axes of the slice: x: 2, y: 2, z: 1, core: 2. Of those that a mesh axis runs over, the one named last changes fastest.
Arguments:
- x_in: bfloat16 [4, 3072, 2048], P('dp', 'sp'), parts along dimension 0
- d_out: bfloat16 [4, 3072, 2048], P('dp', 'sp'), parts along dimension 0
- gain: float32 [2048], replicated
- w_q: bfloat16 [2048, 32, 64], replicated
- w_k: bfloat16 [2048, 8, 64], replicated
- w_v: bfloat16 [2048, 8, 64], replicated
- w_o: bfloat16 [32, 64, 2048], replicated
Outputs:
- output 1: bfloat16 [4, 3072, 2048], P('dp', 'sp'), parts along dimension 0
- output 2: bfloat16 [4, 3072, 2048], P('dp', 'sp'), parts along dimension 0
- output 3: float32 [4096, 32, 64], P('dp'), parts along dimension 0
- output 4: float32 [4096, 8, 64], P('dp'), parts along dimension 0
- output 5: float32 [4096, 8, 64], P('dp'), parts along dimension 0
- output 6: float32 [64, 64, 2048], P('dp'), parts along dimension 0
- output 7: float32 [4096], P('dp'), parts along dimension 0
There are 2 independent parts. The reference program is written for one: setup_inputs(seed, part) draws one part's arguments, and reference() takes and returns one part's arrays. A program takes and returns all parts, laid end to end along the dimension named above; an argument that names none is the same for every part.
All inputs are finite; a program needn't handle non-finite values.
Results may differ from the reference program's by a relative error of at most 0.0124877.
Values are sent between devices in bfloat16 or wider.
A program may use at most 1 GiB of HBM per device.

```python
import jax
import jax.numpy as jnp
from jax import lax

BATCH = 2
SEQ = 3072
D_MODEL = 2048
HEADS = 32
KV_HEADS = 8
HEAD = 64

ROPE_BASE = 1000000.0
NORM_EPS = 1e-5


def setup_inputs(seed: int = 0, part: int = 0) -> dict:
    part_key = jax.random.fold_in(jax.random.key(seed), part)
    key_x, key_dy = jax.random.split(part_key, 2)
    shared = jax.random.split(jax.random.key(seed + 1), 5)
    x_val = jax.random.normal(key_x, (BATCH, SEQ, D_MODEL), jnp.float32)
    dy_val = jax.random.normal(key_dy, (BATCH, SEQ, D_MODEL), jnp.float32)
    gain = jax.random.uniform(shared[0], (D_MODEL,), jnp.float32, 0.6, 1.4)
    in_scale = D_MODEL ** -0.5
    w_q = jax.random.normal(shared[1], (D_MODEL, HEADS, HEAD), jnp.float32) * (1.5 * in_scale)
    w_k = jax.random.normal(shared[2], (D_MODEL, KV_HEADS, HEAD), jnp.float32) * (1.5 * in_scale)
    w_v = jax.random.normal(shared[3], (D_MODEL, KV_HEADS, HEAD), jnp.float32) * in_scale
    w_o = jax.random.normal(shared[4], (HEADS, HEAD, D_MODEL), jnp.float32) * (2.0 * (HEADS * HEAD) ** -0.5)
    return {'x_in': x_val.astype(jnp.bfloat16), 'd_out': dy_val.astype(jnp.bfloat16), 'gain': gain, 'w_q': w_q.astype(jnp.bfloat16), 'w_k': w_k.astype(jnp.bfloat16), 'w_v': w_v.astype(jnp.bfloat16), 'w_o': w_o.astype(jnp.bfloat16)}


def rope_tables(positions):
    half = HEAD // 2
    inv_freq = ROPE_BASE ** (-2.0 * jnp.arange(half, dtype=jnp.float32) / HEAD)
    angle = positions[:, None] * inv_freq[None, :]
    return jnp.cos(angle), jnp.sin(angle)


def rotate(t_val, cos_t, sin_t):
    half = HEAD // 2
    first = t_val[..., :half]
    second = t_val[..., half:]
    cos_b = cos_t[:, None, :]
    sin_b = sin_t[:, None, :]
    return jnp.concatenate([first * cos_b - second * sin_b, second * cos_b + first * sin_b], axis=-1)


def attention(q_all, k_all, v_all):
    group = HEADS // KV_HEADS
    block_len = 128
    num_blocks = SEQ // block_len
    scale = HEAD ** -0.5
    k_f32 = k_all.astype(jnp.float32)
    v_f32 = v_all.astype(jnp.float32)
    q_grouped = jnp.moveaxis(q_all.reshape(BATCH, num_blocks, block_len, KV_HEADS, group, HEAD), 1, 0)
    key_pos = jnp.arange(SEQ)

    def one_block(pair):
        q_rows, block_idx = pair
        scores = jnp.einsum('bqkgd,btkd->bkgqt', q_rows.astype(jnp.float32), k_f32) * scale
        q_pos = block_idx * block_len + jnp.arange(block_len)
        scores = jnp.where(key_pos[None, :] <= q_pos[:, None], scores, -1e30)
        attn_weights = jax.nn.softmax(scores, axis=-1).astype(jnp.bfloat16).astype(jnp.float32)
        out_rows = jnp.einsum('bkgqt,btkd->bqkgd', attn_weights, v_f32)
        return out_rows.astype(jnp.bfloat16)

    out_blocks = lax.map(jax.checkpoint(one_block), (q_grouped, jnp.arange(num_blocks)))
    return jnp.moveaxis(out_blocks, 0, 1).reshape(BATCH, SEQ, HEADS, HEAD)


def block_forward(x_in, gain, w_q, w_k, w_v, w_o):
    x_f32 = x_in.astype(jnp.float32)
    inv_rms = lax.rsqrt(jnp.mean(x_f32 * x_f32, axis=-1, keepdims=True) + NORM_EPS)
    normed = (x_f32 * inv_rms * gain).astype(jnp.bfloat16).astype(jnp.float32)
    cos_t, sin_t = rope_tables(jnp.arange(SEQ, dtype=jnp.float32))
    q_all = rotate(jnp.einsum('btd,dhe->bthe', normed, w_q), cos_t, sin_t).astype(jnp.bfloat16)
    k_all = rotate(jnp.einsum('btd,dhe->bthe', normed, w_k), cos_t, sin_t).astype(jnp.bfloat16)
    v_all = jnp.einsum('btd,dhe->bthe', normed, w_v).astype(jnp.bfloat16)
    mixed = attention(q_all, k_all, v_all)
    y_proj = jnp.einsum('bthe,hed->btd', mixed.astype(jnp.float32), w_o)
    return (x_f32 + y_proj).astype(jnp.bfloat16)


def reference(x_in, d_out, gain, w_q, w_k, w_v, w_o):
    y_out, pullback = jax.vjp(block_forward, x_in, gain, w_q.astype(jnp.float32), w_k.astype(jnp.float32), w_v.astype(jnp.float32), w_o.astype(jnp.float32))
    d_x, d_gain, d_wq, d_wk, d_wv, d_wo = pullback(d_out)
    return (y_out, d_x, d_wq, d_wk, d_wv, d_wo, d_gain)
```

```python
import jax
import jax.numpy as jnp
from jax import lax
from jax.experimental import pallas as pl
from jax.experimental.pallas import tpu as pltpu
from jax.sharding import PartitionSpec as P

ROPE_BASE = 1000000.0
NORM_EPS = 1e-5
HD = 64
GROUP = 4
BQ = 256
WIDE = 512
LOG2E = 1.4426950408889634
NEG = -1e30


def causal_steps(step, q_idx):
    per_wide = WIDE // BQ

    def body(i, carry):
        step(pl.multiple_of(i * WIDE, WIDE), WIDE, False)
        return carry

    wide = q_idx // per_wide
    lax.fori_loop(0, wide, body, 0)

    def tail(i, carry):
        step(pl.multiple_of(i * BQ, BQ), BQ, False)
        return carry

    lax.fori_loop(wide * per_wide, q_idx, tail, 0)
    step(pl.multiple_of(q_idx * BQ, BQ), BQ, True)


def mask_scores(scores):
    rows = lax.broadcasted_iota(jnp.int32, scores.shape, 0)
    cols = lax.broadcasted_iota(jnp.int32, scores.shape, 1)
    return jnp.where(rows <= cols, scores, NEG)


def transpose_rows(src_ref, dst_ref):
    seq = dst_ref.shape[0]

    def body(i, carry):
        start = pl.multiple_of(i * WIDE, WIDE)
        dst_ref[pl.ds(start, WIDE), :] = src_ref[:, pl.ds(start, WIDE)].T
        return carry

    lax.fori_loop(0, seq // WIDE, body, 0)


def fwd_kernel(qt_ref, kt_ref, vt_ref, ot_ref, lse_ref, k_scr, acc_scr, m_scr, l_scr):
    q_idx = pl.program_id(1)

    @pl.when(q_idx == 0)
    def _():
        transpose_rows(kt_ref, k_scr)

    acc_scr[...] = jnp.zeros_like(acc_scr)
    m_scr[...] = jnp.full_like(m_scr, NEG)
    l_scr[...] = jnp.zeros_like(l_scr)
    factor = HD ** -0.5 * LOG2E

    def step(start, width, masked):
        k_rows = k_scr[pl.ds(start, width), :]
        v_cols = vt_ref[:, pl.ds(start, width)]
        m_all = m_scr[...]
        l_all = l_scr[...]
        scores = [jnp.dot(k_rows, qt_ref[g * HD:(g + 1) * HD, :], preferred_element_type=jnp.float32) for g in range(GROUP)]
        if masked:
            scores = [mask_scores(s) for s in scores]
        m_new, l_new, accs = [], [], []
        for g in range(GROUP):
            m_prev = m_all[g:g + 1]
            peak = jnp.maximum(m_prev, jnp.max(scores[g], axis=0, keepdims=True) * factor)
            probs = jnp.exp2(scores[g] * factor - peak)
            alpha = jnp.exp2(m_prev - peak)
            l_new.append(l_all[g:g + 1] * alpha + jnp.sum(probs, axis=0, keepdims=True))
            m_new.append(peak)
            accs.append(acc_scr[g * HD:(g + 1) * HD, :] * alpha + jnp.dot(v_cols, probs.astype(jnp.bfloat16), preferred_element_type=jnp.float32))
        for g in range(GROUP):
            m_scr[g:g + 1, :] = m_new[g]
            l_scr[g:g + 1, :] = l_new[g]
            acc_scr[g * HD:(g + 1) * HD, :] = accs[g]

    causal_steps(step, q_idx)
    lse_ref[0] = m_scr[...] + jnp.log2(jnp.maximum(l_scr[...], 1e-30))
    for g in range(GROUP):
        heads = slice(g * HD, (g + 1) * HD)
        ot_ref[0, heads, :] = (acc_scr[heads, :] / l_scr[g:g + 1, :]).astype(jnp.bfloat16)


def bwd_kernel(qt_ref, kt_ref, vt_ref, dot_ref, ot_ref, lse_ref, cosq_ref, sinq_ref, cos_ref, sin_ref, dqt_ref, dkt_ref, dvt_ref, k_scr, v_scr, dk_scr, dv_scr, dq_scr, q_scr, do_scr, dos_scr, delta_scr):
    q_idx = pl.program_id(1)
    seq = k_scr.shape[0]

    @pl.when(q_idx == 0)
    def _():
        transpose_rows(kt_ref, k_scr)
        transpose_rows(vt_ref, v_scr)
        dk_scr[...] = jnp.zeros_like(dk_scr)
        dv_scr[...] = jnp.zeros_like(dv_scr)

    dq_scr[...] = jnp.zeros_like(dq_scr)
    scale = HD ** -0.5
    factor = scale * LOG2E
    for g in range(GROUP):
        heads = slice(g * HD, (g + 1) * HD)
        do_t = dot_ref[heads, :]
        q_scr[g] = qt_ref[heads, :].T
        do_scr[g] = do_t.T
        do_f32 = do_t.astype(jnp.float32) * scale
        dos_scr[heads, :] = do_f32.astype(jnp.bfloat16)
        delta_scr[g:g + 1, :] = jnp.sum(do_f32 * ot_ref[0, heads, :].astype(jnp.float32), axis=0, keepdims=True)

    def step(start, width, masked):
        rows = pl.ds(start, width)
        k_rows = k_scr[rows, :]
        v_rows = v_scr[rows, :]
        k_cols = kt_ref[:, rows]
        dk_sum = dv_sum = None
        for g in range(GROUP):
            heads = slice(g * HD, (g + 1) * HD)
            scores = jnp.dot(k_rows, qt_ref[heads, :], preferred_element_type=jnp.float32) * factor
            if masked:
                scores = mask_scores(scores)
            probs = jnp.exp2(scores - lse_ref[0, g:g + 1, :])
            d_probs = jnp.dot(v_rows, dos_scr[heads, :], preferred_element_type=jnp.float32).astype(jnp.bfloat16).astype(jnp.float32)
            d_scores = (probs * (d_probs - delta_scr[g:g + 1, :])).astype(jnp.bfloat16)
            dv_part = jnp.dot(probs.astype(jnp.bfloat16), do_scr[g], preferred_element_type=jnp.float32)
            dk_part = jnp.dot(d_scores, q_scr[g], preferred_element_type=jnp.float32)
            dv_sum = dv_part if g == 0 else dv_sum + dv_part
            dk_sum = dk_part if g == 0 else dk_sum + dk_part
            dq_scr[heads, :] = dq_scr[heads, :] + jnp.dot(k_cols, d_scores, preferred_element_type=jnp.float32)
        dv_scr[rows, :] = dv_scr[rows, :] + dv_sum
        dk_scr[rows, :] = dk_scr[rows, :] + dk_sum

    causal_steps(step, q_idx)
    half = HD // 2
    cos_q = cosq_ref[...]
    sin_q = sinq_ref[...]
    for g in range(GROUP):
        grad = dq_scr[g * HD:(g + 1) * HD, :].astype(jnp.bfloat16).astype(jnp.float32)
        first, second = grad[:half], grad[half:]
        dqt_ref[0, g * HD:g * HD + half, :] = (first * cos_q + second * sin_q).astype(jnp.bfloat16)
        dqt_ref[0, g * HD + half:(g + 1) * HD, :] = (second * cos_q - first * sin_q).astype(jnp.bfloat16)

    @pl.when(q_idx == pl.num_programs(1) - 1)
    def _():
        per = dkt_ref.shape[2]
        for j in range(seq // per):
            cols = slice(j * per, (j + 1) * per)
            grad = dk_scr[cols, :].T.astype(jnp.bfloat16).astype(jnp.float32)
            first, second = grad[:half], grad[half:]
            dkt_ref[j, :half, :] = (first * cos_ref[:, cols] + second * sin_ref[:, cols]).astype(jnp.bfloat16)
            dkt_ref[j, half:, :] = (second * cos_ref[:, cols] - first * sin_ref[:, cols]).astype(jnp.bfloat16)
            dvt_ref[j] = dv_scr[cols, :].T.astype(jnp.bfloat16)


def attn_fwd(qt, kt, vt, parts):
    feats, seq = qt.shape
    num_kv = kt.shape[0] // HD
    per = seq // parts
    sub = per // BQ
    rows = GROUP * HD
    pairs = num_kv * GROUP * seq * seq // 2
    return pl.pallas_call(
        fwd_kernel,
        grid=(num_kv, seq // BQ),
        in_specs=[
            pl.BlockSpec((rows, BQ), lambda h, i: (h, i)),
            pl.BlockSpec((HD, seq), lambda h, i: (h, 0)),
            pl.BlockSpec((HD, seq), lambda h, i: (h, 0)),
        ],
        out_specs=[
            pl.BlockSpec((1, rows, BQ), lambda h, i: (i // sub, h, i % sub)),
            pl.BlockSpec((1, 8, BQ), lambda h, i: (h, 0, i)),
        ],
        out_shape=[
            jax.ShapeDtypeStruct((parts, feats, per), jnp.bfloat16),
            jax.ShapeDtypeStruct((num_kv, 8, seq), jnp.float32),
        ],
        scratch_shapes=[
            pltpu.VMEM((seq, HD), jnp.bfloat16),
            pltpu.VMEM((rows, BQ), jnp.float32),
            pltpu.VMEM((8, BQ), jnp.float32),
            pltpu.VMEM((8, BQ), jnp.float32),
        ],
        compiler_params=pltpu.CompilerParams(dimension_semantics=("arbitrary", "arbitrary"), vmem_limit_bytes=40 * 2 ** 20),
        cost_estimate=pl.CostEstimate(flops=pairs * 4 * 256, bytes_accessed=feats * seq * 6, transcendentals=pairs),
        name="attn_fwd",
    )(qt, kt, vt)


def attn_bwd(qt, kt, vt, dot, ot, lse, cos_t, sin_t):
    feats, seq = qt.shape
    num_kv = kt.shape[0] // HD
    parts, _, per = ot.shape
    sub = per // BQ
    rows = GROUP * HD
    half = HD // 2
    pairs = num_kv * GROUP * seq * seq // 2
    q_spec = pl.BlockSpec((rows, BQ), lambda h, i: (h, i))
    kv_spec = pl.BlockSpec((HD, seq), lambda h, i: (h, 0))
    part_spec = pl.BlockSpec((1, rows, BQ), lambda h, i: (i // sub, h, i % sub))
    rope_q = pl.BlockSpec((half, BQ), lambda h, i: (0, i))
    rope_all = pl.BlockSpec((half, seq), lambda h, i: (0, 0))
    dkv_spec = pl.BlockSpec((parts, HD, per), lambda h, i: (0, h, 0))
    return pl.pallas_call(
        bwd_kernel,
        grid=(num_kv, seq // BQ),
        in_specs=[q_spec, kv_spec, kv_spec, q_spec, part_spec, pl.BlockSpec((1, 8, BQ), lambda h, i: (h, 0, i)), rope_q, rope_q, rope_all, rope_all],
        out_specs=[part_spec, dkv_spec, dkv_spec],
        out_shape=[
            jax.ShapeDtypeStruct((parts, feats, per), jnp.bfloat16),
            jax.ShapeDtypeStruct((parts, num_kv * HD, per), jnp.bfloat16),
            jax.ShapeDtypeStruct((parts, num_kv * HD, per), jnp.bfloat16),
        ],
        scratch_shapes=[
            pltpu.VMEM((seq, HD), jnp.bfloat16),
            pltpu.VMEM((seq, HD), jnp.bfloat16),
            pltpu.VMEM((seq, HD), jnp.float32),
            pltpu.VMEM((seq, HD), jnp.float32),
            pltpu.VMEM((rows, BQ), jnp.float32),
            pltpu.VMEM((GROUP, BQ, HD), jnp.bfloat16),
            pltpu.VMEM((GROUP, BQ, HD), jnp.bfloat16),
            pltpu.VMEM((rows, BQ), jnp.bfloat16),
            pltpu.VMEM((8, BQ), jnp.float32),
        ],
        compiler_params=pltpu.CompilerParams(dimension_semantics=("arbitrary", "arbitrary"), vmem_limit_bytes=48 * 2 ** 20),
        cost_estimate=pl.CostEstimate(flops=pairs * 10 * 256, bytes_accessed=feats * seq * 10, transcendentals=pairs),
        name="attn_bwd",
    )(qt, kt, vt, dot, ot, lse, cos_t, sin_t, cos_t, sin_t)


def rope_tables(seq, head_dim):
    half = head_dim // 2
    inv_freq = ROPE_BASE ** (-2.0 * jnp.arange(half, dtype=jnp.float32) / head_dim)
    angle = inv_freq[:, None] * jnp.arange(seq, dtype=jnp.float32)[None, :]
    return jnp.cos(angle), jnp.sin(angle)


def rotate(lin, cos_t, sin_t):
    feats, seq = lin.shape
    half = HD // 2
    pairs = lin.reshape(feats // HD, 2, half, seq)
    first, second = pairs[:, 0], pairs[:, 1]
    turned = jnp.stack([first * cos_t - second * sin_t, second * cos_t + first * sin_t], axis=1)
    return turned.reshape(feats, seq).astype(jnp.bfloat16)


def dot32(spec, lhs, rhs):
    return jnp.einsum(spec, lhs, rhs, preferred_element_type=jnp.float32)


def solution(mesh):
    parts = mesh.shape['sp']

    def local_step(x_local, dy_local, gain, w_q, w_k, w_v, w_o):
        batch, seq_loc, d_model = x_local.shape
        seq = seq_loc * parts
        q_feats = w_q.shape[1] * HD // parts
        kv_feats = w_k.shape[1] * HD // parts
        idx = lax.axis_index('sp')

        def own(w):
            heads = w.shape[1] // parts
            return lax.dynamic_slice_in_dim(w, idx * heads, heads, axis=1).reshape(d_model, heads * HD)

        x_f32 = x_local.astype(jnp.float32)
        inv_rms = lax.rsqrt(jnp.mean(x_f32 * x_f32, axis=-1, keepdims=True) + NORM_EPS)
        normed = (x_f32 * inv_rms * gain).astype(jnp.bfloat16)

        r_all = [lax.all_gather(normed[b], 'sp', axis=0, tiled=True) for b in range(batch)]
        dy_all = [lax.all_gather(dy_local[b], 'sp', axis=0, tiled=True) for b in range(batch)]

        w_own = jnp.concatenate([own(w_q), own(w_k), own(w_v)], axis=1)
        w_cat = jnp.concatenate([w.reshape(d_model, parts, -1) for w in (w_q, w_k, w_v)], axis=2)
        w_o2 = w_o.reshape(parts, q_feats, d_model)
        w_o_own = lax.dynamic_index_in_dim(w_o2, idx, axis=0, keepdims=False)
        cos_t, sin_t = rope_tables(seq, HD)

        qkv, outs, y_rows = [], [], []
        for b in range(batch):
            lin = dot32('df,td->ft', w_own, r_all[b])
            q_t = rotate(lin[:q_feats], cos_t, sin_t)
            k_t = rotate(lin[q_feats:q_feats + kv_feats], cos_t, sin_t)
            v_t = lin[q_feats + kv_feats:].astype(jnp.bfloat16)
            o_t, lse = attn_fwd(q_t, k_t, v_t, parts)
            qkv.append((q_t, k_t, v_t))
            outs.append((o_t, lse))
            o_all = lax.all_to_all(o_t, 'sp', 0, 0, tiled=True)
            y_rows.append(dot32('jft,jfd->td', o_all, w_o2))
        y_out = (x_f32 + jnp.stack(y_rows)).astype(jnp.bfloat16)

        d_wo = None
        d_wqkv = None
        d_rows = []
        for b in range(batch):
            o_t, lse = outs[b]
            dy_parts = dy_all[b].reshape(parts, seq_loc, d_model)
            part = dot32('jft,jtd->fd', o_t, dy_parts)
            d_wo = part if d_wo is None else d_wo + part
        d_wo = lax.all_gather(d_wo, 'sp', axis=0, tiled=True)
        for b in range(batch):
            o_t, lse = outs[b]
            do_t = dot32('fd,td->ft', w_o_own, dy_all[b]).astype(jnp.bfloat16)
            grads = attn_bwd(*qkv[b], do_t, o_t, lse, cos_t, sin_t)
            d_qkv = jnp.concatenate(grads, axis=1)
            d_all = lax.all_to_all(d_qkv, 'sp', 0, 0, tiled=True)
            d_rows.append(dot32('jft,djf->td', d_all, w_cat))
            part = dot32('jtd,jft->df', r_all[b].reshape(parts, seq_loc, d_model), d_qkv)
            d_wqkv = part if d_wqkv is None else d_wqkv + part
        d_wqkv = lax.all_gather(d_wqkv, 'sp', axis=0)
        d_wqkv = jnp.moveaxis(d_wqkv, 0, 1)
        d_wq = d_wqkv[:, :, :q_feats].reshape(d_model, -1, HD)
        d_wk = d_wqkv[:, :, q_feats:q_feats + kv_feats].reshape(d_model, -1, HD)
        d_wv = d_wqkv[:, :, q_feats + kv_feats:].reshape(d_model, -1, HD)

        d_normed = jnp.stack(d_rows).astype(jnp.bfloat16).astype(jnp.float32)
        x_hat = x_f32 * inv_rms
        d_hat = d_normed * gain
        d_norm = inv_rms * (d_hat - x_hat * jnp.mean(d_hat * x_hat, axis=-1, keepdims=True))
        d_x = (dy_local.astype(jnp.float32) + d_norm).astype(jnp.bfloat16)
        d_gain = lax.psum(jnp.sum(d_normed * x_hat, axis=(0, 1)), 'sp')
        return y_out, d_x, d_wq, d_wk, d_wv, d_wo.reshape(-1, HD, d_model), d_gain

    specs_in = (P('dp', 'sp', None), P('dp', 'sp', None), P(None), P(None, None, None), P(None, None, None), P(None, None, None), P(None, None, None))
    specs_out = (P('dp', 'sp', None), P('dp', 'sp', None), P('dp', None, None), P('dp', None, None), P('dp', None, None), P('dp', None, None), P('dp'))
    return jax.shard_map(local_step, mesh=mesh, in_specs=specs_in, out_specs=specs_out, check_vma=False)
```
